32 devices in a mesh: row: 8 (over z, x), col: 4 (over y, core).
Axes of the slice: x: 2, y: 2, z: 4, core: 2. Of those that a mesh axis runs over, the one named last changes fastest.
Arguments:
- queries: bfloat16 [8192, 2048], P(('row', 'col')), may hold values from -200 to 200
- keys: bfloat16 [8192, 512], P(('row', 'col')), may hold values from -6 to 6
- values: bfloat16 [8192, 512], P(('row', 'col')), may hold values from -6 to 6
- mid_key_weight: bfloat16 [1024, 128], replicated, may hold values from -0.1875 to 0.1875
- mid_value_weight: bfloat16 [1024, 128], replicated, may hold values from -0.1875 to 0.1875
- far_key_weight: bfloat16 [2048, 128], replicated, may hold values from -0.125 to 0.125
- far_value_weight: bfloat16 [2048, 128], replicated, may hold values from -0.125 to 0.125
Outputs:
- attended: bfloat16 [8192, 2048], P(('row', 'col'))
The draws below stay inside these ranges and needn't reach their ends.
All inputs are finite; a program needn't handle non-finite values.
Results may differ from the reference program's by a relative error of at most 0.012.
Values may be sent and summed in bfloat16 or wider, within the bound.
A program may use at most 128 MiB of HBM per device.

```python
import jax
import jax.numpy as jnp
from jax import lax

HQ = 16
HK = 4
DH = 128
BLOCK = 512
MID = 8
FAR = 16
TOK_DEV = 256
TOKENS = 8192
N_ROW = 8
N_COL = 4
DEVICES = 32


def draw_queries(key, part):
    key_one = jax.random.fold_in(key, 0)
    normal_part = jnp.clip(jax.random.normal(key_one, (TOKENS, HQ * DH), jnp.float32), -6.0, 6.0)
    return (1.5 * normal_part).astype(jnp.bfloat16)


def block_levels(own_key, extent, cuts, low, largest):
    factor_of, own = 1.0, jax.random.fold_in(own_key, 6)
    for axis_at, shards_of in cuts:
        heights = jnp.exp(jax.random.uniform(jax.random.fold_in(own, axis_at), (shards_of,), jnp.float32, low / len(cuts), largest / len(cuts)))
        factor_of = factor_of * jnp.repeat(heights, extent[axis_at] // shards_of).reshape([-1 if axis == axis_at else 1 for axis in range(len(extent))])
    return factor_of


def centred(own_key, shape, spread, most, cuts=(), kind=jnp.bfloat16):
    entries = spread * jax.random.normal(own_key, shape, jnp.float32)
    if cuts:
        entries = entries * block_levels(own_key, shape, cuts, -0.22, 0.18)
    return jnp.clip(entries, -most, most).astype(kind)


def setup_inputs(seed: int = 0) -> dict:
    splits = jax.random.split(jax.random.key(seed), 8)
    return {
        "queries": draw_queries(jax.random.fold_in(splits[7], 71), 0),
        "keys": centred(splits[1], (TOKENS, HK * DH), 1.0, 6.0, ((0, 32),)),
        "values": centred(splits[2], (TOKENS, HK * DH), 1.0, 6.0, ((0, 32),)),
        "mid_key_weight": centred(splits[3], (MID * DH, DH), (MID * DH) ** -0.5, 0.1875),
        "mid_value_weight": centred(splits[4], (MID * DH, DH), (MID * DH) ** -0.5, 0.1875),
        "far_key_weight": centred(splits[5], (FAR * DH, DH), (FAR * DH) ** -0.5, 0.125),
        "far_value_weight": centred(splits[6], (FAR * DH, DH), (FAR * DH) ** -0.5, 0.125),
    }


NEG_FILL = -1e30


def squeeze_groups(source, weight, squeeze):
    group_count = source.shape[0] // squeeze
    grouped = source.reshape(group_count, squeeze, HK, DH).transpose(0, 2, 1, 3).reshape(group_count, HK, squeeze * DH)
    merged = jnp.einsum("nhr,rd->nhd", grouped.astype(jnp.float32), weight.astype(jnp.float32))
    return merged.astype(jnp.bfloat16).reshape(group_count, HK * DH)


def attend(queries, keys, values, visible):
    group_size = HQ // HK
    query_rows = queries.shape[0]
    query4 = queries.reshape(query_rows, HK, group_size, DH).astype(jnp.float32)
    key_heads = keys.reshape(keys.shape[0], HK, DH).astype(jnp.float32)
    value_heads = values.reshape(values.shape[0], HK, DH).astype(jnp.float32)
    scores = jnp.einsum("thgd,shd->hgts", query4, key_heads) * (DH ** -0.5)
    top_score = jnp.max(jnp.where(visible, scores, NEG_FILL), axis=-1, keepdims=True)
    weights = jnp.exp(jnp.where(visible, scores - top_score, NEG_FILL))
    weight_sum = jnp.sum(weights, axis=-1)
    rounded = lax.optimization_barrier(weights.astype(jnp.bfloat16))
    mixed_out = jnp.einsum("hgts,shd->thgd", rounded.astype(jnp.float32), value_heads)
    weight_sum = jnp.transpose(weight_sum, (2, 0, 1))[..., None]
    return (mixed_out / jnp.maximum(weight_sum, 1.0)).reshape(query_rows, HQ * DH)


def reference(queries, keys, values, mid_key_weight, mid_value_weight, far_key_weight, far_value_weight):
    tok_rows = TOK_DEV
    mid_keys = squeeze_groups(keys, mid_key_weight, MID)
    mid_values = squeeze_groups(values, mid_value_weight, MID)
    far_keys = squeeze_groups(keys, far_key_weight, FAR)
    far_values = squeeze_groups(values, far_value_weight, FAR)
    row_mid = N_COL * tok_rows // MID
    row_far = N_COL * tok_rows // FAR
    zero_rows = jnp.zeros((3 * tok_rows, HK * DH), keys.dtype)
    padded_keys = jnp.concatenate([zero_rows, keys], axis=0)
    padded_values = jnp.concatenate([zero_rows, values], axis=0)
    far_row = jnp.arange(N_ROW * row_far, dtype=jnp.int32) // row_far

    def one_tile(device_pos):
        first_pos = device_pos * tok_rows
        query_pos = first_pos + jnp.arange(tok_rows, dtype=jnp.int32)
        query_tile = lax.dynamic_slice_in_dim(queries, first_pos, tok_rows, 0)
        near_keys = lax.dynamic_slice_in_dim(padded_keys, first_pos, 4 * tok_rows, 0)
        near_values = lax.dynamic_slice_in_dim(padded_values, first_pos, 4 * tok_rows, 0)
        key_pos = first_pos - 3 * tok_rows + jnp.arange(4 * tok_rows, dtype=jnp.int32)
        near_seen = (key_pos[None, :] <= query_pos[:, None]) & (key_pos[None, :] >= 0) & (key_pos[None, :] // BLOCK >= query_pos[:, None] // BLOCK - 1)
        grid_row = device_pos // N_COL
        row_first = grid_row * (N_COL * tok_rows)
        mid_k = lax.dynamic_slice_in_dim(mid_keys, grid_row * row_mid, row_mid, 0)
        mid_v = lax.dynamic_slice_in_dim(mid_values, grid_row * row_mid, row_mid, 0)
        mid_end = row_first + MID * jnp.arange(row_mid, dtype=jnp.int32) + MID - 1
        mid_seen = mid_end[None, :] <= query_pos[:, None]
        far_seen = jnp.broadcast_to(far_row[None, :] < grid_row, (tok_rows, N_ROW * row_far))
        summed = attend(query_tile, near_keys, near_values, near_seen)
        summed = summed + attend(query_tile, mid_k, mid_v, mid_seen)
        summed = summed + attend(query_tile, far_keys, far_values, far_seen)
        return summed.astype(jnp.bfloat16)

    all_tiles = lax.map(one_tile, jnp.arange(DEVICES, dtype=jnp.int32))
    return all_tiles.reshape(DEVICES * tok_rows, HQ * DH)
```

```python
import functools
import math

import jax
import jax.numpy as jnp
from jax import lax
from jax.experimental import pallas as pl
from jax.experimental.pallas import tpu as pltpu
from jax.sharding import PartitionSpec as P

HQ = 16
HK = 4
DH = 128
BLOCK = 512
MID = 8
FAR = 16
GROUP = HQ // HK
KV = HK * DH
NEG_FILL = -1e30
EXP_SCALE = DH ** (-0.5) * math.log2(math.e)
FAR_CHUNK = 512
MESH = pl.DeviceIdType.MESH
FROM_PARTNER, FROM_BEHIND, RELAYED = 0, 1, 2


def score(q, k):
    return lax.dot_general(q, k, (((1,), (1,)), ((), ())), preferred_element_type=jnp.float32)


def weigh(p, v):
    both = jnp.concatenate([v, jnp.ones_like(v)], axis=1)
    return jnp.dot(p.astype(jnp.bfloat16), both, preferred_element_type=jnp.float32)


def powers(s, top):
    return jnp.exp2((s - top) * EXP_SCALE)


def normalised(acc):
    return acc[:, :DH] / jnp.maximum(acc[:, DH:], 1.0)


def kernel(
    rows, cols,
    q_ref, k_ref, v_ref, wmk_ref, wmv_ref, wfk_ref, wfv_ref, out_ref,
    wide, mid_buf, far_own, far_buf, near, top_ref, acc_ref, rest_ref,
    near_send, near_recv, mid_send, mid_recv,
    f1_send, f1_recv, f2_send, f2_recv, f3_send, f3_recv,
):
    tok = q_ref.shape[0]
    mids, fars = tok // MID, tok // FAR
    total = rows * cols
    pairs = cols // 2
    row, col = lax.axis_index("row"), lax.axis_index("col")
    pos = row * cols + col
    side = lax.rem(col, 2)
    pair = col // 2
    other = col + 1 - 2 * side
    partner = (row, other)

    def at(linear):
        return (linear // cols, lax.rem(linear, cols))

    mid_buf[...] = jnp.zeros_like(mid_buf)

    def clear(c, _):
        far_buf[c] = jnp.zeros(far_buf.shape[1:], far_buf.dtype)
        return 0

    lax.fori_loop(0, cols, clear, 0)

    barrier = pltpu.get_barrier_semaphore()

    def greet(device):
        pl.semaphore_signal(barrier, inc=1, device_id=device, device_id_type=MESH)

    def greet_col(i, _):
        greet((row, lax.rem(col + i, cols)))
        return 0

    def greet_row(i, _):
        greet((lax.rem(row + i, rows), col))
        return 0

    lax.fori_loop(1, cols, greet_col, 0)
    lax.fori_loop(1, rows, greet_row, 0)
    greet(at(lax.rem(pos + 2, total)))
    greet(at(lax.rem(pos + total - 2, total)))

    mid_rows = pl.ds(pl.multiple_of(col * mids, mids), mids)
    for s, (src, wm, wf) in enumerate(((k_ref, wmk_ref, wfk_ref), (v_ref, wmv_ref, wfv_ref))):
        for h in range(HK):
            wide[s * HK + h] = src[:, h * DH:(h + 1) * DH].astype(jnp.float32)
        for squeeze, count, weight in ((FAR, fars, wf), (MID, mids, wm)):
            grouped = jnp.concatenate(
                [
                    jnp.concatenate(
                        [wide[s * HK + h, pl.ds(i, count, stride=squeeze), :] for h in range(HK)],
                        axis=0,
                    ).astype(jnp.bfloat16)
                    for i in range(squeeze)
                ],
                axis=1,
            )
            merged = jnp.dot(grouped, weight[...], preferred_element_type=jnp.float32)
            merged = merged.astype(jnp.bfloat16)
            for h in range(HK):
                lanes = slice(s * KV + h * DH, s * KV + (h + 1) * DH)
                piece = merged[h * count:(h + 1) * count]
                if squeeze == FAR:
                    far_own[:, lanes] = piece
                else:
                    mid_buf[mid_rows, lanes] = piece

    pl.semaphore_wait(barrier, cols + rows)

    def remote(src, dst, send, recv, device):
        return pltpu.make_async_remote_copy(
            src_ref=src, dst_ref=dst, send_sem=send, recv_sem=recv,
            device_id=device, device_id_type=MESH,
        )

    def far_slot(c, r):
        return far_buf.at[c, pl.ds(pl.multiple_of(r * fars, fars), fars), :]

    def far1(r_to, r_from):
        return remote(far_own, far_slot(col, r_from), f1_send.at[r_to], f1_recv.at[r_from], (r_to, col))

    def far2(r, p_to, p_from):
        return remote(
            far_slot(2 * p_from + side, r), far_slot(2 * p_from + side, r),
            f2_send.at[p_to, r], f2_recv.at[p_from, r], (row, 2 * p_to + side),
        )

    def far3(r, p, s):
        return remote(
            far_slot(2 * p + s, r), far_slot(2 * p + s, r),
            f3_send.at[p, r], f3_recv.at[p, r], partner,
        )

    def mid_copy(c_to, c_from):
        span = mid_buf.at[pl.ds(pl.multiple_of(c_from * mids, mids), mids), :]
        return remote(span, span, mid_send.at[c_to], mid_recv.at[c_from], (row, c_to))

    def near_copy(slot, i, src, device):
        return remote(
            src, near.at[slot, i], near_send.at[slot, i], near_recv.at[slot, i], device
        )

    own = (k_ref, v_ref)
    ahead = at(lax.rem(pos + 2, total))

    def loop(low, high, f):
        def step(i, _):
            f(i)
            return 0

        lax.fori_loop(low, high, step, 0)

    loop(row + 1, rows, lambda r: far1(r, row).start())
    loop(col + 1, cols, lambda c: mid_copy(c, col).start())

    @pl.when(side == 0)
    def _():
        for i in range(2):
            near_copy(FROM_PARTNER, i, own[i], partner).start()

    @pl.when(pos + 2 < total)
    def _():
        for i in range(2):
            near_copy(FROM_BEHIND, i, own[i], ahead).start()

    def head_lanes(h, base=0):
        return pl.ds(pl.multiple_of(base + h * DH, DH), DH)

    def query_of(h):
        q = q_ref[:, pl.ds(pl.multiple_of(h * GROUP * DH, DH), GROUP * DH)]
        return jnp.concatenate([q[:, g * DH:(g + 1) * DH] for g in range(GROUP)], axis=0)

    def tiled_mask(seen, s):
        lines, keys = seen.shape
        shaped = s.reshape(GROUP, lines, keys)
        return shaped, seen[None]

    def masked(seen, s, fill):
        shaped, seen = tiled_mask(seen, s)
        return jnp.where(seen, shaped, fill).reshape(s.shape)

    def iota(shape, axis):
        return lax.broadcasted_iota(jnp.int32, shape, axis)

    def near_first(with_partner):
        def one(h):
            q = query_of(h)
            seen = iota((tok, tok), 1) <= iota((tok, tok), 0)
            s = masked(seen, score(q, k_ref[:, head_lanes(h)]), NEG_FILL)
            top = jnp.max(s, axis=-1, keepdims=True)
            if with_partner:
                s2 = score(q, near[FROM_PARTNER, 0, :, head_lanes(h)])
                top = jnp.maximum(top, jnp.max(s2, axis=-1, keepdims=True))
            acc = weigh(powers(s, top), v_ref[:, head_lanes(h)])
            if with_partner:
                acc = acc + weigh(powers(s2, top), near[FROM_PARTNER, 1, :, head_lanes(h)])
            acc_ref[h] = acc
            top_ref[h] = top

        loop(0, HK, one)

    @pl.when(side == 0)
    def _():
        near_first(False)

    def pass_on(r):
        far1(r, r).wait_recv()

        def to_pair(p):
            @pl.when(p != pair)
            def _():
                far2(r, p, pair).start()

        loop(0, pairs, to_pair)
        far3(r, pair, side).start()

    def far_pass():
        loop(0, row, pass_on)

    @pl.when(side == 0)
    def _():
        far_pass()

    @pl.when(side == 1)
    def _():
        for i in range(2):
            near_copy(FROM_PARTNER, i, own[i], partner).wait_recv()
        near_first(True)
        far_pass()

    loop(0, col, lambda c: mid_copy(c, c).wait_recv())
    n_mid = mid_buf.shape[0]

    def mid_one(h):
        q = query_of(h)
        seen = (iota((tok, n_mid), 1) * MID + MID - 1) <= (iota((tok, n_mid), 0) + col * tok)
        s = masked(seen, score(q, mid_buf[:, head_lanes(h)]), NEG_FILL)
        top = jnp.max(s, axis=-1, keepdims=True)
        p = masked(seen, powers(s, top), 0.0)
        rest_ref[h] = normalised(weigh(p, mid_buf[:, head_lanes(h, KV)]))

    loop(0, HK, mid_one)

    def pass_partner(r):
        def from_pair(p):
            @pl.when(p != pair)
            def _():
                far2(r, p, p).wait_recv()
                far3(r, p, side).start()

        loop(0, pairs, from_pair)

    loop(0, row, pass_partner)
    loop(0, row, lambda r: loop(0, pairs, lambda p: far3(r, p, 1 - side).wait_recv()))

    line = far_buf.shape[1]
    per = max(1, min(cols, FAR_CHUNK // line))
    n_chunk = cols // per

    def far_one(h):
        q = query_of(h)
        seen = lax.rem(iota((1, per * line), 1), line) < row * fars

        def part(j, base):
            block = far_buf[pl.ds(j * per, per), :, head_lanes(h, base)]
            return block.reshape(per * line, DH)

        def chunk(j, carry):
            s = jnp.where(seen, score(q, part(j, 0)), NEG_FILL)
            top = jnp.max(s, axis=-1, keepdims=True)
            if carry is None:
                return top, weigh(powers(s, top), part(j, KV))
            before, acc = carry
            top = jnp.maximum(before, top)
            return top, acc * powers(before, top) + weigh(powers(s, top), part(j, KV))

        carry = chunk(0, None)
        if n_chunk > 1:
            carry = lax.fori_loop(1, n_chunk, chunk, carry)
        rest_ref[h] = rest_ref[h] + normalised(carry[1])

    @pl.when(row > 0)
    def _():
        loop(0, HK, far_one)

    def put(h, value):
        for g in range(GROUP):
            lanes = pl.ds(pl.multiple_of((h * GROUP + g) * DH, DH), DH)
            out_ref[:, lanes] = value[g * tok:(g + 1) * tok].astype(out_ref.dtype)

    @pl.when(pos < 2)
    def _():
        loop(0, HK, lambda h: put(h, normalised(acc_ref[h]) + rest_ref[h]))

    @pl.when(pos >= 2)
    def _():
        for i in range(2):
            near_copy(FROM_BEHIND, i, own[i], ahead).wait_recv()
            near_copy(RELAYED, i, near.at[FROM_BEHIND, i], partner).start()
        for i in range(2):
            near_copy(RELAYED, i, near.at[FROM_BEHIND, i], partner).wait_recv()

        def one(h):
            q = query_of(h)
            before = top_ref[h]
            s1 = score(q, near[FROM_BEHIND, 0, :, head_lanes(h)])
            s2 = score(q, near[RELAYED, 0, :, head_lanes(h)])
            top = jnp.maximum(
                before,
                jnp.max(jnp.maximum(s1, s2), axis=-1, keepdims=True),
            )
            acc = acc_ref[h] * powers(before, top)
            acc = acc + weigh(powers(s1, top), near[FROM_BEHIND, 1, :, head_lanes(h)])
            acc = acc + weigh(powers(s2, top), near[RELAYED, 1, :, head_lanes(h)])
            put(h, normalised(acc) + rest_ref[h])

        loop(0, HK, one)

    loop(row + 1, rows, lambda r: far1(r, row).wait_send())
    loop(col + 1, cols, lambda c: mid_copy(c, col).wait_send())

    def sent(r):
        def one(p):
            far3(r, p, side).wait_send()

            @pl.when(p != pair)
            def _():
                far2(r, p, pair).wait_send()

        loop(0, pairs, one)

    loop(0, row, sent)

    @pl.when(side == 0)
    def _():
        for i in range(2):
            near_copy(FROM_PARTNER, i, own[i], partner).wait_send()

    @pl.when(pos + 2 < total)
    def _():
        for i in range(2):
            near_copy(FROM_BEHIND, i, own[i], ahead).wait_send()

    @pl.when(pos >= 2)
    def _():
        for i in range(2):
            near_copy(RELAYED, i, near.at[FROM_BEHIND, i], partner).wait_send()


def body(rows, cols, queries, keys, values, *weights):
    tok = queries.shape[0]
    assert BLOCK == 2 * tok and cols % 2 == 0
    dma = pltpu.SemaphoreType.DMA
    bf16, f32 = jnp.bfloat16, jnp.float32
    lines = GROUP * tok
    vmem = pl.BlockSpec(memory_space=pltpu.VMEM)
    return pl.pallas_call(
        functools.partial(kernel, rows, cols),
        out_shape=jax.ShapeDtypeStruct(queries.shape, bf16),
        in_specs=[vmem] * 7,
        out_specs=vmem,
        scratch_shapes=[
            pltpu.VMEM((2 * HK, tok, DH), f32),
            pltpu.VMEM((cols * (tok // MID), 2 * KV), bf16),
            pltpu.VMEM((tok // FAR, 2 * KV), bf16),
            pltpu.VMEM((cols, rows * (tok // FAR), 2 * KV), bf16),
            pltpu.VMEM((3, 2, tok, KV), bf16),
            pltpu.VMEM((HK, lines, 1), f32),
            pltpu.VMEM((HK, lines, 2 * DH), f32),
            pltpu.VMEM((HK, lines, DH), f32),
            dma((3, 2)),
            dma((3, 2)),
            dma((cols,)),
            dma((cols,)),
            dma((rows,)),
            dma((rows,)),
            dma((cols // 2, rows)),
            dma((cols // 2, rows)),
            dma((cols // 2, rows)),
            dma((cols // 2, rows)),
        ],
        compiler_params=pltpu.CompilerParams(
            collective_id=0, has_side_effects=True, vmem_limit_bytes=60 * 1024 * 1024
        ),
    )(queries, keys, values, *weights)


def solution(mesh):
    spec = P(("row", "col"), None)
    return jax.shard_map(
        functools.partial(body, mesh.shape["row"], mesh.shape["col"]),
        mesh=mesh,
        in_specs=(spec, spec, spec, P(), P(), P(), P()),
        out_specs=spec,
        check_vma=False,
    )
```

```python
import functools
import math

import jax
import jax.numpy as jnp
from jax import lax
from jax.experimental import pallas as pl
from jax.experimental.pallas import tpu as pltpu
from jax.sharding import PartitionSpec as P

HQ = 16
HK = 4
DH = 128
BLOCK = 512
MID = 8
FAR = 16
GROUP = HQ // HK
KV = HK * DH
NEG_FILL = -1e30
EXP_SCALE = DH ** (-0.5) * math.log2(math.e)
FAR_CHUNK = 512
VMEM_LIMIT = 60 * 1024 * 1024
MESH = pl.DeviceIdType.MESH
FROM_PARTNER, FROM_BEHIND, RELAYED = 0, 1, 2


def score(q, k):
    return lax.dot_general(q, k, (((1,), (1,)), ((), ())), preferred_element_type=jnp.float32)


def weigh(p, v):
    both = jnp.concatenate([v, jnp.ones_like(v)], axis=1)
    return jnp.dot(p.astype(jnp.bfloat16), both, preferred_element_type=jnp.float32)


def powers(s, top):
    return jnp.exp2((s - top) * EXP_SCALE)


def normalised(acc):
    return acc[:, :DH] / jnp.maximum(acc[:, DH:], 1.0)


def kernel(
    rows, cols,
    q_hbm, k_hbm, v_hbm, wmk_hbm, wmv_hbm, wfk_hbm, wfv_hbm, out_ref,
    q_ref, k_ref, v_ref, wmk_ref, wmv_ref, wfk_ref, wfv_ref, fetch_sem,
    wide, mid_buf, far_own, far_buf, near, top_ref, acc_ref, rest_ref,
    near_send, near_recv, mid_send, mid_recv,
    f1_send, f1_recv, f2_send, f2_recv, f3_send, f3_recv,
):
    tok = q_ref.shape[0]
    mids, fars = tok // MID, tok // FAR
    total = rows * cols
    pairs = cols // 2
    row, col = lax.axis_index("row"), lax.axis_index("col")
    pos = row * cols + col
    side = lax.rem(col, 2)
    pair = col // 2
    other = col + 1 - 2 * side
    partner = (row, other)

    def fetch(i, src, dst):
        return pltpu.make_async_copy(src, dst, fetch_sem.at[i])

    fetches = [
        fetch(i, src, dst)
        for i, (src, dst) in enumerate((
            (k_hbm, k_ref), (wfk_hbm, wfk_ref), (wmk_hbm, wmk_ref),
            (v_hbm, v_ref), (wfv_hbm, wfv_ref), (wmv_hbm, wmv_ref), (q_hbm, q_ref),
        ))
    ]
    for copy in fetches:
        copy.start()

    def at(linear):
        return (linear // cols, lax.rem(linear, cols))

    mid_buf[...] = jnp.zeros_like(mid_buf)

    def clear(c, _):
        far_buf[c] = jnp.zeros(far_buf.shape[1:], far_buf.dtype)
        return 0

    lax.fori_loop(0, cols, clear, 0)

    barrier = pltpu.get_barrier_semaphore()

    def greet(device):
        pl.semaphore_signal(barrier, inc=1, device_id=device, device_id_type=MESH)

    def greet_col(i, _):
        greet((row, lax.rem(col + i, cols)))
        return 0

    def greet_row(i, _):
        greet((lax.rem(row + i, rows), col))
        return 0

    lax.fori_loop(1, cols, greet_col, 0)
    lax.fori_loop(1, rows, greet_row, 0)
    greet(at(lax.rem(pos + 2, total)))
    greet(at(lax.rem(pos + total - 2, total)))


    def head_lanes(h, base=0):
        return pl.ds(pl.multiple_of(base + h * DH, DH), DH)

    def remote(src, dst, send, recv, device):
        return pltpu.make_async_remote_copy(
            src_ref=src, dst_ref=dst, send_sem=send, recv_sem=recv,
            device_id=device, device_id_type=MESH,
        )

    def far_slot(c, r):
        return far_buf.at[c, pl.ds(pl.multiple_of(r * fars, fars), fars), :]

    def far1(r_to, r_from):
        return remote(far_own, far_slot(col, r_from), f1_send.at[r_to], f1_recv.at[r_from], (r_to, col))

    def far2(r, p_to, p_from):
        return remote(
            far_slot(2 * p_from + side, r), far_slot(2 * p_from + side, r),
            f2_send.at[p_to, r], f2_recv.at[p_from, r], (row, 2 * p_to + side),
        )

    def far3(r, p, s):
        return remote(
            far_slot(2 * p + s, r), far_slot(2 * p + s, r),
            f3_send.at[p, r], f3_recv.at[p, r], partner,
        )

    def mid_copy(c_to, c_from):
        span = mid_buf.at[pl.ds(pl.multiple_of(c_from * mids, mids), mids), :]
        return remote(span, span, mid_send.at[c_to], mid_recv.at[c_from], (row, c_to))

    def near_copy(slot, i, src, device):
        return remote(
            src, near.at[slot, i], near_send.at[slot, i, 0], near_recv.at[slot, i, 0], device
        )

    def behind_copy(i, h):
        lanes = head_lanes(h)
        return remote(
            own[i].at[:, lanes], near.at[FROM_BEHIND, i, :, lanes],
            near_send.at[FROM_BEHIND, i, h], near_recv.at[FROM_BEHIND, i, h], ahead,
        )

    def relay_copy(i, h):
        lanes = head_lanes(h)
        return remote(
            near.at[FROM_BEHIND, i, :, lanes], near.at[RELAYED, i, :, lanes],
            near_send.at[RELAYED, i, h], near_recv.at[RELAYED, i, h], partner,
        )

    def behind_start(h):
        for i in range(2):
            behind_copy(i, h).start()

    own = (k_ref, v_ref)
    ahead = at(lax.rem(pos + 2, total))

    def loop(low, high, f):
        def step(i, _):
            f(i)
            return 0

        lax.fori_loop(low, high, step, 0)

    mid_rows = pl.ds(pl.multiple_of(col * mids, mids), mids)

    def summarise(s, src, wm, wf):
        for copy in fetches[4 * s:3 * s + 3]:
            copy.wait()
        for h in range(HK):
            wide[s * HK + h] = src[:, h * DH:(h + 1) * DH].astype(jnp.float32)
        for squeeze, count, weight in ((FAR, fars, wf), (MID, mids, wm)):
            grouped = jnp.concatenate(
                [
                    jnp.concatenate(
                        [wide[s * HK + h, pl.ds(i, count, stride=squeeze), :] for h in range(HK)],
                        axis=0,
                    ).astype(jnp.bfloat16)
                    for i in range(squeeze)
                ],
                axis=1,
            )
            merged = jnp.dot(grouped, weight[...], preferred_element_type=jnp.float32)
            merged = merged.astype(jnp.bfloat16)
            for h in range(HK):
                lanes = slice(s * KV + h * DH, s * KV + (h + 1) * DH)
                piece = merged[h * count:(h + 1) * count]
                if squeeze == FAR:
                    far_own[:, lanes] = piece
                else:
                    mid_buf[mid_rows, lanes] = piece

    summarise(0, k_ref, wmk_ref, wfk_ref)
    fetches[3].wait()
    pl.semaphore_wait(barrier, cols + rows)

    @pl.when(pos + 2 < total)
    def _():
        behind_start(0)

    summarise(1, v_ref, wmv_ref, wfv_ref)

    loop(row + 1, rows, lambda r: far1(r, row).start())
    loop(col + 1, cols, lambda c: mid_copy(c, col).start())

    @pl.when(side == 0)
    def _():
        for i in range(2):
            near_copy(FROM_PARTNER, i, own[i], partner).start()

    @pl.when(pos + 2 < total)
    def _():
        loop(1, HK, behind_start)

    fetches[6].wait()

    def query_of(h):
        q = q_ref[:, pl.ds(pl.multiple_of(h * GROUP * DH, DH), GROUP * DH)]
        return jnp.concatenate([q[:, g * DH:(g + 1) * DH] for g in range(GROUP)], axis=0)

    def queries_of(h):
        base = h * GROUP * DH
        return [
            q_ref[:, pl.ds(pl.multiple_of(base + g * DH, DH), DH)] for g in range(GROUP)
        ]

    def tiled_mask(seen, s):
        lines, keys = seen.shape
        shaped = s.reshape(GROUP, lines, keys)
        return shaped, seen[None]

    def masked(seen, s, fill):
        shaped, seen = tiled_mask(seen, s)
        return jnp.where(seen, shaped, fill).reshape(s.shape)

    def iota(shape, axis):
        return lax.broadcasted_iota(jnp.int32, shape, axis)

    def near_first(with_partner):
        def one(h):
            seen = iota((tok, tok), 1) <= iota((tok, tok), 0)
            key_parts = [k_ref[:, head_lanes(h)]]
            value_parts = [v_ref[:, head_lanes(h)]]
            if with_partner:
                key_parts.append(near[FROM_PARTNER, 0, :, head_lanes(h)])
                value_parts.append(near[FROM_PARTNER, 1, :, head_lanes(h)])
            s = [[score(q, k) for k in key_parts] for q in queries_of(h)]
            for g, parts in enumerate(s):
                parts = [jnp.where(seen, parts[0], NEG_FILL)] + parts[1:]
                top = jnp.max(functools.reduce(jnp.maximum, parts), axis=-1, keepdims=True)
                span = slice(g * tok, (g + 1) * tok)
                terms = [weigh(powers(p, top), v) for p, v in zip(parts, value_parts)]
                acc_ref[h, span] = functools.reduce(jnp.add, terms)
                top_ref[h, span] = top

        loop(0, HK, one)

    @pl.when(side == 0)
    def _():
        near_first(False)

    def pass_on(r):
        far1(r, r).wait_recv()

        def to_pair(p):
            @pl.when(p != pair)
            def _():
                far2(r, p, pair).start()

        loop(0, pairs, to_pair)
        far3(r, pair, side).start()

    def far_pass():
        loop(0, row, pass_on)

    @pl.when(side == 0)
    def _():
        far_pass()

    @pl.when(side == 1)
    def _():
        for i in range(2):
            near_copy(FROM_PARTNER, i, own[i], partner).wait_recv()
        near_first(True)
        far_pass()

    loop(0, col, lambda c: mid_copy(c, c).wait_recv())
    n_mid = mid_buf.shape[0]

    def mid_one(h):
        q = query_of(h)
        seen = (iota((tok, n_mid), 1) * MID + MID - 1) <= (iota((tok, n_mid), 0) + col * tok)
        s = masked(seen, score(q, mid_buf[:, head_lanes(h)]), NEG_FILL)
        top = jnp.max(s, axis=-1, keepdims=True)
        p = masked(seen, powers(s, top), 0.0)
        rest_ref[h] = normalised(weigh(p, mid_buf[:, head_lanes(h, KV)]))

    loop(0, HK // 2, mid_one)

    def pass_partner(r):
        def from_pair(p):
            @pl.when(p != pair)
            def _():
                far2(r, p, p).wait_recv()
                far3(r, p, side).start()

        loop(0, pairs, from_pair)

    loop(0, row, pass_partner)
    loop(HK // 2, HK, mid_one)
    loop(0, row, lambda r: loop(0, pairs, lambda p: far3(r, p, 1 - side).wait_recv()))

    line = far_buf.shape[1]
    per = max(1, min(cols, FAR_CHUNK // line))
    n_chunk = cols // per

    def far_one(h):
        q = query_of(h)
        seen = lax.rem(iota((1, per * line), 1), line) < row * fars

        def part(j, base):
            block = far_buf[pl.ds(j * per, per), :, head_lanes(h, base)]
            return block.reshape(per * line, DH)

        def chunk(j, carry):
            s = jnp.where(seen, score(q, part(j, 0)), NEG_FILL)
            top = jnp.max(s, axis=-1, keepdims=True)
            if carry is None:
                return top, weigh(powers(s, top), part(j, KV))
            before, acc = carry
            top = jnp.maximum(before, top)
            return top, acc * powers(before, top) + weigh(powers(s, top), part(j, KV))

        carry = chunk(0, None)
        if n_chunk > 1:
            carry = lax.fori_loop(1, n_chunk, chunk, carry)
        rest_ref[h] = rest_ref[h] + normalised(carry[1])

    def put(h, g, value):
        lanes = pl.ds(pl.multiple_of((h * GROUP + g) * DH, DH), DH)
        out_ref[:, lanes] = value.astype(out_ref.dtype)

    def arrive(h):
        for i in range(2):
            behind_copy(i, h).wait_recv()
            relay_copy(i, h).start()

    def near_last(h):
        for i in range(2):
            relay_copy(i, h).wait_recv()
        parts = (FROM_BEHIND, RELAYED)
        s = [
            [score(q, near[slot, 0, :, head_lanes(h)]) for slot in parts]
            for q in queries_of(h)
        ]
        for g, pair_s in enumerate(s):
            span = slice(g * tok, (g + 1) * tok)
            before = top_ref[h, span]
            top = jnp.maximum(before, jnp.max(jnp.maximum(*pair_s), axis=-1, keepdims=True))
            acc = acc_ref[h, span] * powers(before, top)
            for slot, part in zip(parts, pair_s):
                acc = acc + weigh(powers(part, top), near[slot, 1, :, head_lanes(h)])
            put(h, g, normalised(acc) + rest_ref[h, span])

    def far_step(h):
        @pl.when(row > 0)
        def _():
            far_one(h)

    lead = HK // 2
    loop(0, lead, far_step)

    @pl.when(pos >= 2)
    def _():
        arrive(0)

    def step(h):
        @pl.when(h + lead < HK)
        def _():
            far_step(h + lead)

        @pl.when((pos >= 2) & (h + 1 < HK))
        def _():
            arrive(h + 1)

        @pl.when(pos >= 2)
        def _():
            near_last(h)

    loop(0, HK, step)

    @pl.when(pos < 2)
    def _():
        def one(h):
            for g in range(GROUP):
                span = slice(g * tok, (g + 1) * tok)
                put(h, g, normalised(acc_ref[h, span]) + rest_ref[h, span])

        loop(0, HK, one)

    loop(row + 1, rows, lambda r: far1(r, row).wait_send())
    loop(col + 1, cols, lambda c: mid_copy(c, col).wait_send())

    def sent(r):
        def one(p):
            far3(r, p, side).wait_send()

            @pl.when(p != pair)
            def _():
                far2(r, p, pair).wait_send()

        loop(0, pairs, one)

    loop(0, row, sent)

    @pl.when(side == 0)
    def _():
        for i in range(2):
            near_copy(FROM_PARTNER, i, own[i], partner).wait_send()

    @pl.when(pos + 2 < total)
    def _():
        for i in range(2):
            loop(0, HK, lambda h, i=i: behind_copy(i, h).wait_send())

    @pl.when(pos >= 2)
    def _():
        for i in range(2):
            loop(0, HK, lambda h, i=i: relay_copy(i, h).wait_send())


def body(rows, cols, queries, keys, values, *weights):
    tok = queries.shape[0]
    assert BLOCK == 2 * tok and cols % 2 == 0
    dma = pltpu.SemaphoreType.DMA
    bf16, f32 = jnp.bfloat16, jnp.float32
    lines = GROUP * tok
    vmem = pl.BlockSpec(memory_space=pltpu.VMEM)
    return pl.pallas_call(
        functools.partial(kernel, rows, cols),
        out_shape=jax.ShapeDtypeStruct(queries.shape, bf16),
        in_specs=[pl.BlockSpec(memory_space=pltpu.HBM)] * 7,
        out_specs=vmem,
        scratch_shapes=[
            *[pltpu.VMEM(a.shape, a.dtype) for a in (queries, keys, values, *weights)],
            dma((7,)),
            pltpu.VMEM((2 * HK, tok, DH), f32),
            pltpu.VMEM((cols * (tok // MID), 2 * KV), bf16),
            pltpu.VMEM((tok // FAR, 2 * KV), bf16),
            pltpu.VMEM((cols, rows * (tok // FAR), 2 * KV), bf16),
            pltpu.VMEM((3, 2, tok, KV), bf16),
            pltpu.VMEM((HK, lines, 1), f32),
            pltpu.VMEM((HK, lines, 2 * DH), f32),
            pltpu.VMEM((HK, lines, DH), f32),
            dma((3, 2, HK)),
            dma((3, 2, HK)),
            dma((cols,)),
            dma((cols,)),
            dma((rows,)),
            dma((rows,)),
            dma((cols // 2, rows)),
            dma((cols // 2, rows)),
            dma((cols // 2, rows)),
            dma((cols // 2, rows)),
        ],
        compiler_params=pltpu.CompilerParams(
            collective_id=0, has_side_effects=True, vmem_limit_bytes=VMEM_LIMIT
        ),
    )(queries, keys, values, *weights)


def solution(mesh):
    spec = P(("row", "col"), None)
    return jax.shard_map(
        functools.partial(body, mesh.shape["row"], mesh.shape["col"]),
        mesh=mesh,
        in_specs=(spec, spec, spec, P(), P(), P(), P()),
        out_specs=spec,
        check_vma=False,
    )
```

```python
import functools
import math

import jax
import jax.numpy as jnp
from jax import lax
from jax.experimental import pallas as pl
from jax.experimental.pallas import tpu as pltpu
from jax.sharding import PartitionSpec as P

HQ = 16
HK = 4
DH = 128
BLOCK = 512
MID = 8
FAR = 16
GROUP = HQ // HK
KV = HK * DH
NEG_FILL = -1e30
EXP_SCALE = DH ** (-0.5) * math.log2(math.e)
FAR_CHUNK = 512
VMEM_LIMIT = 57 * 1024 * 1024
MESH = pl.DeviceIdType.MESH
FROM_PARTNER, FROM_BEHIND, RELAYED = 0, 1, 2


def score(q, k):
    return lax.dot_general(q, k, (((1,), (1,)), ((), ())), preferred_element_type=jnp.float32)


def weigh(p, v):
    both = jnp.concatenate([v, jnp.ones_like(v)], axis=1)
    return jnp.dot(p.astype(jnp.bfloat16), both, preferred_element_type=jnp.float32)


def powers(s, top):
    return jnp.exp2((s - top) * EXP_SCALE)


def normalised(acc):
    return acc[:, :DH] / jnp.maximum(acc[:, DH:], 1.0)


def kernel(
    rows, cols,
    q_hbm, k_hbm, v_hbm, wmk_hbm, wmv_hbm, wfk_hbm, wfv_hbm, out_ref,
    q_ref, k_ref, v_ref, wmk_ref, wmv_ref, wfk_ref, wfv_ref, fetch_sem,
    wide, mid_buf, far_own, far_buf, near, top_ref, acc_ref, rest_ref,
    near_send, near_recv, mid_send, mid_recv,
    f1_send, f1_recv, f2_send, f2_recv, f3_send, f3_recv,
):
    tok = q_ref.shape[0]
    mids, fars = tok // MID, tok // FAR
    total = rows * cols
    pairs = cols // 2
    row, col = lax.axis_index("row"), lax.axis_index("col")
    pos = row * cols + col
    side = lax.rem(col, 2)
    pair = col // 2
    other = col + 1 - 2 * side
    partner = (row, other)

    def fetch(i, src, dst):
        return pltpu.make_async_copy(src, dst, fetch_sem.at[i])

    fetches = [
        fetch(i, src, dst)
        for i, (src, dst) in enumerate((
            (k_hbm, k_ref), (wfk_hbm, wfk_ref), (wmk_hbm, wmk_ref),
            (v_hbm, v_ref), (wfv_hbm, wfv_ref), (wmv_hbm, wmv_ref), (q_hbm, q_ref),
        ))
    ]
    for copy in fetches:
        copy.start()

    def at(linear):
        return (linear // cols, lax.rem(linear, cols))

    mid_buf[...] = jnp.zeros_like(mid_buf)

    def clear(c, _):
        far_buf[c] = jnp.zeros(far_buf.shape[1:], far_buf.dtype)
        return 0

    lax.fori_loop(0, cols, clear, 0)

    barrier = pltpu.get_barrier_semaphore()

    def greet(device):
        pl.semaphore_signal(barrier, inc=1, device_id=device, device_id_type=MESH)

    def greet_col(i, _):
        greet((row, lax.rem(col + i, cols)))
        return 0

    def greet_row(i, _):
        greet((lax.rem(row + i, rows), col))
        return 0

    lax.fori_loop(1, cols, greet_col, 0)
    lax.fori_loop(1, rows, greet_row, 0)
    greet(at(lax.rem(pos + 2, total)))
    greet(at(lax.rem(pos + total - 2, total)))


    def head_lanes(h, base=0):
        return pl.ds(pl.multiple_of(base + h * DH, DH), DH)

    def remote(src, dst, send, recv, device):
        return pltpu.make_async_remote_copy(
            src_ref=src, dst_ref=dst, send_sem=send, recv_sem=recv,
            device_id=device, device_id_type=MESH,
        )

    def far_slot(c, r):
        return far_buf.at[c, pl.ds(pl.multiple_of(r * fars, fars), fars), :]

    def far1(r_to, r_from):
        return remote(far_own, far_slot(col, r_from), f1_send.at[r_to], f1_recv.at[r_from], (r_to, col))

    def far2(r, p_to, p_from):
        return remote(
            far_slot(2 * p_from + side, r), far_slot(2 * p_from + side, r),
            f2_send.at[p_to, r], f2_recv.at[p_from, r], (row, 2 * p_to + side),
        )

    def far3(r, p, s):
        return remote(
            far_slot(2 * p + s, r), far_slot(2 * p + s, r),
            f3_send.at[p, r], f3_recv.at[p, r], partner,
        )

    def mid_copy(c_to, c_from):
        span = mid_buf.at[pl.ds(pl.multiple_of(c_from * mids, mids), mids), :]
        return remote(span, span, mid_send.at[c_to], mid_recv.at[c_from], (row, c_to))

    def near_copy(slot, i, src, device):
        return remote(
            src, near.at[slot, i], near_send.at[slot, i, 0], near_recv.at[slot, i, 0], device
        )

    def behind_copy(i, h):
        lanes = head_lanes(h)
        return remote(
            own[i].at[:, lanes], near.at[FROM_BEHIND, i, :, lanes],
            near_send.at[FROM_BEHIND, i, h], near_recv.at[FROM_BEHIND, i, h], ahead,
        )

    def relay_copy(i, h):
        lanes = head_lanes(h)
        return remote(
            near.at[FROM_BEHIND, i, :, lanes], near.at[RELAYED, i, :, lanes],
            near_send.at[RELAYED, i, h], near_recv.at[RELAYED, i, h], partner,
        )

    def behind_start(h):
        for i in range(2):
            behind_copy(i, h).start()

    own = (k_ref, v_ref)
    ahead = at(lax.rem(pos + 2, total))

    def loop(low, high, f):
        def step(i, _):
            f(i)
            return 0

        lax.fori_loop(low, high, step, 0)

    mid_rows = pl.ds(pl.multiple_of(col * mids, mids), mids)

    def summarise(s, src, wm, wf):
        for copy in fetches[4 * s:3 * s + 3]:
            copy.wait()
        for h in range(HK):
            wide[s * HK + h] = src[:, h * DH:(h + 1) * DH].astype(jnp.float32)
        for squeeze, count, weight in ((FAR, fars, wf), (MID, mids, wm)):
            grouped = jnp.concatenate(
                [
                    jnp.concatenate(
                        [wide[s * HK + h, pl.ds(i, count, stride=squeeze), :] for h in range(HK)],
                        axis=0,
                    ).astype(jnp.bfloat16)
                    for i in range(squeeze)
                ],
                axis=1,
            )
            merged = jnp.dot(grouped, weight[...], preferred_element_type=jnp.float32)
            merged = merged.astype(jnp.bfloat16)
            for h in range(HK):
                lanes = slice(s * KV + h * DH, s * KV + (h + 1) * DH)
                piece = merged[h * count:(h + 1) * count]
                if squeeze == FAR:
                    far_own[:, lanes] = piece
                else:
                    mid_buf[mid_rows, lanes] = piece

    summarise(0, k_ref, wmk_ref, wfk_ref)
    fetches[3].wait()
    pl.semaphore_wait(barrier, cols + rows)

    @pl.when(pos + 2 < total)
    def _():
        behind_start(0)

    summarise(1, v_ref, wmv_ref, wfv_ref)

    loop(row + 1, rows, lambda r: far1(r, row).start())
    loop(col + 1, cols, lambda c: mid_copy(c, col).start())

    @pl.when(side == 0)
    def _():
        for i in range(2):
            near_copy(FROM_PARTNER, i, own[i], partner).start()

    @pl.when(pos + 2 < total)
    def _():
        loop(1, HK, behind_start)

    fetches[6].wait()

    def query_of(h):
        q = q_ref[:, pl.ds(pl.multiple_of(h * GROUP * DH, DH), GROUP * DH)]
        return jnp.concatenate([q[:, g * DH:(g + 1) * DH] for g in range(GROUP)], axis=0)

    def queries_of(h):
        base = h * GROUP * DH
        return [
            q_ref[:, pl.ds(pl.multiple_of(base + g * DH, DH), DH)] for g in range(GROUP)
        ]

    def tiled_mask(seen, s):
        lines, keys = seen.shape
        shaped = s.reshape(GROUP, lines, keys)
        return shaped, seen[None]

    def masked(seen, s, fill):
        shaped, seen = tiled_mask(seen, s)
        return jnp.where(seen, shaped, fill).reshape(s.shape)

    def iota(shape, axis):
        return lax.broadcasted_iota(jnp.int32, shape, axis)

    def near_first(with_partner):
        def one(h):
            seen = iota((tok, tok), 1) <= iota((tok, tok), 0)
            key_parts = [k_ref[:, head_lanes(h)]]
            value_parts = [v_ref[:, head_lanes(h)]]
            if with_partner:
                key_parts.append(near[FROM_PARTNER, 0, :, head_lanes(h)])
                value_parts.append(near[FROM_PARTNER, 1, :, head_lanes(h)])
            s = [[score(q, k) for k in key_parts] for q in queries_of(h)]
            for g, parts in enumerate(s):
                parts = [jnp.where(seen, parts[0], NEG_FILL)] + parts[1:]
                top = jnp.max(functools.reduce(jnp.maximum, parts), axis=-1, keepdims=True)
                span = slice(g * tok, (g + 1) * tok)
                terms = [weigh(powers(p, top), v) for p, v in zip(parts, value_parts)]
                acc_ref[h, span] = functools.reduce(jnp.add, terms)
                top_ref[h, span] = top

        loop(0, HK, one)

    @pl.when(side == 0)
    def _():
        near_first(False)

    def pass_on(r):
        far1(r, r).wait_recv()

        def to_pair(p):
            @pl.when(p != pair)
            def _():
                far2(r, p, pair).start()

        loop(0, pairs, to_pair)
        far3(r, pair, side).start()

    def far_pass():
        loop(0, row, pass_on)

    @pl.when(side == 0)
    def _():
        far_pass()

    @pl.when(side == 1)
    def _():
        for i in range(2):
            near_copy(FROM_PARTNER, i, own[i], partner).wait_recv()
        near_first(True)
        far_pass()

    loop(0, col, lambda c: mid_copy(c, c).wait_recv())
    n_mid = mid_buf.shape[0]

    def mid_one(h):
        q = query_of(h)
        seen = (iota((tok, n_mid), 1) * MID + MID - 1) <= (iota((tok, n_mid), 0) + col * tok)
        s = masked(seen, score(q, mid_buf[:, head_lanes(h)]), NEG_FILL)
        top = jnp.max(s, axis=-1, keepdims=True)
        p = masked(seen, powers(s, top), 0.0)
        rest_ref[h] = normalised(weigh(p, mid_buf[:, head_lanes(h, KV)]))

    loop(0, HK // 2, mid_one)

    def pass_partner(r):
        def from_pair(p):
            @pl.when(p != pair)
            def _():
                far2(r, p, p).wait_recv()
                far3(r, p, side).start()

        loop(0, pairs, from_pair)

    loop(0, row, pass_partner)
    loop(HK // 2, HK, mid_one)
    loop(0, row, lambda r: loop(0, pairs, lambda p: far3(r, p, 1 - side).wait_recv()))

    line = far_buf.shape[1]
    per = max(1, min(cols, FAR_CHUNK // line))
    n_chunk = cols // per

    def far_one(h):
        q = query_of(h)
        seen = lax.rem(iota((1, per * line), 1), line) < row * fars

        def part(j, base):
            block = far_buf[pl.ds(j * per, per), :, head_lanes(h, base)]
            return block.reshape(per * line, DH)

        def chunk(j, carry):
            s = jnp.where(seen, score(q, part(j, 0)), NEG_FILL)
            top = jnp.max(s, axis=-1, keepdims=True)
            if carry is None:
                return top, weigh(powers(s, top), part(j, KV))
            before, acc = carry
            top = jnp.maximum(before, top)
            return top, acc * powers(before, top) + weigh(powers(s, top), part(j, KV))

        carry = chunk(0, None)
        if n_chunk > 1:
            carry = lax.fori_loop(1, n_chunk, chunk, carry)
        rest_ref[h] = rest_ref[h] + normalised(carry[1])

    def put(h, g, value):
        lanes = pl.ds(pl.multiple_of((h * GROUP + g) * DH, DH), DH)
        out_ref[:, lanes] = value.astype(out_ref.dtype)

    def arrive(h):
        for i in range(2):
            behind_copy(i, h).wait_recv()
            relay_copy(i, h).start()

    def near_last(h):
        for i in range(2):
            relay_copy(i, h).wait_recv()
        parts = (FROM_BEHIND, RELAYED)
        s = [
            [score(q, near[slot, 0, :, head_lanes(h)]) for slot in parts]
            for q in queries_of(h)
        ]
        for g, pair_s in enumerate(s):
            span = slice(g * tok, (g + 1) * tok)
            before = top_ref[h, span]
            top = jnp.maximum(before, jnp.max(jnp.maximum(*pair_s), axis=-1, keepdims=True))
            acc = acc_ref[h, span] * powers(before, top)
            for slot, part in zip(parts, pair_s):
                acc = acc + weigh(powers(part, top), near[slot, 1, :, head_lanes(h)])
            put(h, g, normalised(acc) + rest_ref[h, span])

    def far_step(h):
        @pl.when(row > 0)
        def _():
            far_one(h)

    lead = HK // 2
    loop(0, lead, far_step)

    @pl.when(pos >= 2)
    def _():
        arrive(0)

    def step(h):
        @pl.when(h + lead < HK)
        def _():
            far_step(h + lead)

        @pl.when((pos >= 2) & (h + 1 < HK))
        def _():
            arrive(h + 1)

        @pl.when(pos >= 2)
        def _():
            near_last(h)

    loop(0, HK, step)

    @pl.when(pos < 2)
    def _():
        def one(h):
            for g in range(GROUP):
                span = slice(g * tok, (g + 1) * tok)
                put(h, g, normalised(acc_ref[h, span]) + rest_ref[h, span])

        loop(0, HK, one)

    loop(row + 1, rows, lambda r: far1(r, row).wait_send())
    loop(col + 1, cols, lambda c: mid_copy(c, col).wait_send())

    def sent(r):
        def one(p):
            far3(r, p, side).wait_send()

            @pl.when(p != pair)
            def _():
                far2(r, p, pair).wait_send()

        loop(0, pairs, one)

    loop(0, row, sent)

    @pl.when(side == 0)
    def _():
        for i in range(2):
            near_copy(FROM_PARTNER, i, own[i], partner).wait_send()

    @pl.when(pos + 2 < total)
    def _():
        for i in range(2):
            loop(0, HK, lambda h, i=i: behind_copy(i, h).wait_send())

    @pl.when(pos >= 2)
    def _():
        for i in range(2):
            loop(0, HK, lambda h, i=i: relay_copy(i, h).wait_send())


def body(rows, cols, queries, keys, values, *weights):
    tok = queries.shape[0]
    assert BLOCK == 2 * tok and cols % 2 == 0
    dma = pltpu.SemaphoreType.DMA
    bf16, f32 = jnp.bfloat16, jnp.float32
    lines = GROUP * tok
    vmem = pl.BlockSpec(memory_space=pltpu.VMEM)
    return pl.pallas_call(
        functools.partial(kernel, rows, cols),
        out_shape=pltpu.VMEM(queries.shape, bf16),
        in_specs=[pl.BlockSpec(memory_space=pltpu.HBM)] * 7,
        out_specs=vmem,
        scratch_shapes=[
            *[pltpu.VMEM(a.shape, a.dtype) for a in (queries, keys, values, *weights)],
            dma((7,)),
            pltpu.VMEM((2 * HK, tok, DH), f32),
            pltpu.VMEM((cols * (tok // MID), 2 * KV), bf16),
            pltpu.VMEM((tok // FAR, 2 * KV), bf16),
            pltpu.VMEM((cols, rows * (tok // FAR), 2 * KV), bf16),
            pltpu.VMEM((3, 2, tok, KV), bf16),
            pltpu.VMEM((HK, lines, 1), f32),
            pltpu.VMEM((HK, lines, 2 * DH), f32),
            pltpu.VMEM((HK, lines, DH), f32),
            dma((3, 2, HK)),
            dma((3, 2, HK)),
            dma((cols,)),
            dma((cols,)),
            dma((rows,)),
            dma((rows,)),
            dma((cols // 2, rows)),
            dma((cols // 2, rows)),
            dma((cols // 2, rows)),
            dma((cols // 2, rows)),
        ],
        compiler_params=pltpu.CompilerParams(
            collective_id=0, has_side_effects=True, vmem_limit_bytes=VMEM_LIMIT
        ),
    )(queries, keys, values, *weights)


def solution(mesh):
    spec = P(("row", "col"), None)
    return jax.shard_map(
        functools.partial(body, mesh.shape["row"], mesh.shape["col"]),
        mesh=mesh,
        in_specs=(spec, spec, spec, P(), P(), P(), P()),
        out_specs=spec,
        check_vma=False,
    )
```
